32 devices in a mesh: rep: 4 (over z), exp: 4 (over x, core), shard: 2 (over y).
Axes of the slice: x: 2, y: 2, z: 4, core: 2. Of those that a mesh axis runs over, the one named last changes fastest.
Arguments:
- tokens: bfloat16 [3584, 2048], P(('rep', 'exp', 'shard')), may hold values from -1.5 to 1.5
- routes: int32 [3584, 2], P(('rep', 'exp', 'shard')), may hold values from 0 to 3, all different within a row; in each aligned block of 112 rows (0 to 111, 112 to 223, ...) at most 63 rows name the same one
- gate_weight: bfloat16 [4, 2048, 7168], P('exp', None, 'shard'), may hold values from -0.125 to 0.125
- gate_cotangent: bfloat16 [4, 2016, 7168], P('exp', 'rep', 'shard'), may hold values from -0.75 to 0.75
Outputs:
- token_grad: bfloat16 [3584, 2048], P(('rep', 'exp', 'shard'))
- weight_grad: bfloat16 [4, 2048, 7168], P('exp', None, 'shard')
The draws below stay inside these ranges and needn't reach their ends.
Inputs may be any that keep to these rules, and one draw needn't show every extreme that they name: `routes`: the two entries of a row differ. The rows of one device name one expert at most 63 times, and some device names some expert exactly 63 times.
All inputs are finite; a program needn't handle non-finite values.
Results may differ from the reference program's by a relative error of at most 0.015.
Values may be sent and summed in bfloat16 or wider, within the bound.
No kernel may reach another device: no remote copies, remote signals or barrier semaphores. Data moves between devices by JAX's collectives and lax.ppermute only.
A program may use at most 128 MiB of HBM per device.

```python
import math
import jax
import jax.numpy as jnp
import numpy as np
from jax import lax

DW = 2048
FFW = 7168
TOK_DEV = 112
EXPERTS = 4
TOKENS = 3584
SLOT_CAP = 63
SLOTS = 2016
N_REP = 4
N_EXP = 4
N_SHARD = 2


def shard_levels(rng, extent, pieces, least, high):
    gain = 1.0
    for dim, parts in pieces:
        steps = jax.random.uniform(jax.random.fold_in(jax.random.fold_in(rng, 6), dim), (parts,), jnp.float32, least / len(pieces), high / len(pieces))
        gain = gain * jnp.repeat(jnp.exp(steps), extent[dim] // parts).reshape((-1,) + (1,) * (len(extent) - 1 - dim))
    return gain


def routed_block(stream_key, own, number, rows, amount, top, most, lean):
    sequence = jax.random.permutation(stream_key, amount)
    packed, common = load_shares(amount, rows * top, most, lean, True), load_shares(amount, rows * top, most, lean, False)
    places = jnp.arange(amount)

    def named(tallies, rotation):
        used = int((tallies > 0).sum())
        fixed = max(1, used // 4)
        moved = fixed + (places - fixed + rotation * (used - fixed)) % max(1, amount - fixed)
        return jnp.zeros((amount,), jnp.int32).at[sequence[jnp.where(places < fixed, places, moved)]].set(jnp.asarray(tallies, jnp.int32))

    tallies = jnp.where(number % 4 == 0, named(packed, number // 4), named(common, number - number // 4 - 1))
    mixed = jax.random.permutation(jax.random.fold_in(own, 3), amount)
    source_of, taker = mixed[0:amount // 2 * 2:2], mixed[1:amount // 2 * 2:2]
    margin = jnp.minimum(tallies[source_of] - 1, most - tallies[taker]) // 2
    margin = jnp.where((source_of == sequence[0]) | (taker == sequence[0]) | (tallies[taker] == 0), 0, jnp.maximum(margin, 0))
    moved = jax.random.randint(jax.random.fold_in(own, 4), (amount // 2,), 0, 1 << 20) % (margin + 1)
    tallies = tallies.at[source_of].add(-moved).at[taker].add(moved)
    items = jnp.searchsorted(jnp.cumsum(tallies), jnp.arange(rows * top), side="right").astype(jnp.int32)
    listing = items.reshape(top, rows).T
    listing = listing[jax.random.permutation(jax.random.fold_in(own, 1), rows)]
    rotation = jax.random.randint(jax.random.fold_in(own, 2), (rows, 1), 0, top)
    return jnp.take_along_axis(listing, (jnp.arange(top)[None, :] + rotation) % top, axis=1)


def load_shares(number_of, total, limit, slope, full):
    portions = [(1 << 20) // math.isqrt(grade ** slope) + 1 for grade in range(1, number_of + 1)]
    largest = limit if full else min(limit, max(-(-total // number_of), total * portions[0] // sum(portions)))
    least = 1 if total - largest >= number_of - 1 else 0
    holding, surplus = [largest] + [least] * (number_of - 1), total - largest - least * (number_of - 1)
    while surplus > 0:
        free = [i for i in range(1, number_of) if holding[i] < largest] or [i for i in range(1, number_of) if holding[i] < limit]
        mass, left = sum([portions[i] for i in free]), surplus
        for i in free:
            more = min(limit - holding[i], max(1, left * portions[i] // mass), surplus)
            holding[i] = holding[i] + more
            surplus = surplus - more
    return np.array(holding)


def scatter_about(key, dims, spread, limit, split=(), kind=jnp.bfloat16):
    values = spread * jax.random.normal(key, dims, jnp.float32)
    if split:
        values = values * shard_levels(key, dims, split, -0.22, 0.18)
    return jnp.clip(values, -limit, limit).astype(kind)


def setup_inputs(seed: int = 0) -> dict:
    key_list = jax.random.split(jax.random.key(seed), 5)
    tokens = scatter_about(key_list[0], (TOKENS, DW), 0.25, 1.5, ((0, 32),))
    routes_keys = jax.random.split(jax.random.fold_in(key_list[1], 1), TOKENS // TOK_DEV)
    routes_turns = jax.random.permutation(jax.random.fold_in(key_list[1], 3), TOKENS // TOK_DEV)
    routes = jax.vmap(lambda own, number: routed_block(jax.random.fold_in(key_list[1], 2), own, number, TOK_DEV, EXPERTS, 2, SLOT_CAP, 2))(routes_keys, routes_turns).reshape((TOKENS, 2))
    gate_weight = scatter_about(key_list[2], (EXPERTS, DW, FFW), DW ** -0.5, 0.125, ((0, 4), (2, 2)))
    gate_cotangent = scatter_about(key_list[3], (EXPERTS, SLOTS, FFW), 0.125, 0.75, ((0, 4), (1, 4), (2, 2)))
    return {"tokens": tokens, "routes": routes, "gate_weight": gate_weight, "gate_cotangent": gate_cotangent}


def slot_matrix(route_rows, experts, slot_cap):
    expert_ids = jnp.arange(experts, dtype=jnp.int32)
    onehot = (route_rows[:, :, None] == expert_ids[None, None, :]).astype(jnp.int32)
    flattened = onehot.reshape(-1, experts)
    before = jnp.cumsum(flattened, axis=0) - flattened
    position = jnp.sum(before * flattened, axis=1)
    target = jnp.sum(flattened * expert_ids[None, :], axis=1) * slot_cap + position
    slot_ids = jnp.arange(experts * slot_cap, dtype=jnp.int32)
    matches = (target[None, :] == slot_ids[:, None]).astype(jnp.int32)
    return matches.reshape(experts * slot_cap, -1, 2).sum(axis=2)


def reference(tokens, routes, gate_weight, gate_cotangent):
    devices = N_REP * N_EXP * N_SHARD
    token_blocks = tokens.reshape(devices, TOK_DEV, DW).astype(jnp.float32)
    route_blocks = routes.reshape(devices, TOK_DEV, 2)

    def placing_of(route_rows):
        return slot_matrix(route_rows, EXPERTS, SLOT_CAP)

    placing = jax.vmap(placing_of)(route_blocks).astype(jnp.float32)
    outgoing = jnp.einsum("dst,dtw->dsw", placing, token_blocks).astype(jnp.bfloat16)
    grouped = outgoing.reshape(N_REP, N_EXP, N_SHARD, EXPERTS, SLOT_CAP, DW)
    grouped = grouped.transpose(3, 0, 1, 2, 4, 5).reshape(EXPERTS, SLOTS, DW)
    hidden_part = FFW // N_SHARD

    def per_expert(operands):
        gathered, cotangent, weights = operands
        weight_grad = jnp.dot(gathered.T, cotangent, preferred_element_type=jnp.float32).astype(jnp.bfloat16)
        summed = jnp.zeros((SLOTS, DW), jnp.float32)
        for shard_index in range(N_SHARD):
            lower = shard_index * hidden_part
            partial_value = jnp.dot(cotangent[:, lower:lower + hidden_part], weights[:, lower:lower + hidden_part].T,
                              preferred_element_type=jnp.float32).astype(jnp.bfloat16)
            partial_value = lax.optimization_barrier(partial_value)
            summed = summed + partial_value.astype(jnp.float32)
        return weight_grad, summed.astype(jnp.bfloat16)

    weight_grad, slot_grad = lax.map(per_expert, (grouped, gate_cotangent, gate_weight))
    returned = slot_grad.reshape(EXPERTS, N_REP, N_EXP, N_SHARD, SLOT_CAP, DW)
    returned = returned.transpose(1, 2, 3, 0, 4, 5).reshape(devices, EXPERTS * SLOT_CAP, DW)
    token_grad = jnp.einsum("dst,dsw->dtw", placing, returned.astype(jnp.float32)).astype(jnp.bfloat16)
    return token_grad.reshape(TOKENS, DW), weight_grad
```

```python
import functools

import jax
import jax.numpy as jnp
from jax import lax
from jax.experimental import pallas as pl
from jax.experimental.pallas import tpu as pltpu
from jax.sharding import PartitionSpec as P


ROW_TILE = 256
BOUNDS = (0, 2, 4, 6, 7)


def slot_matrix(route_rows, experts, slot_cap):
    expert_ids = jnp.arange(experts, dtype=jnp.int32)
    onehot = (route_rows[:, :, None] == expert_ids[None, None, :]).astype(jnp.int32)
    named = onehot.sum(axis=1)
    rows = named.shape[0]
    earlier = (jnp.arange(rows)[:, None] > jnp.arange(rows)[None, :]).astype(jnp.bfloat16)
    before = jnp.dot(earlier, named.astype(jnp.bfloat16), preferred_element_type=jnp.float32)
    position = jnp.where(named > 0, before.astype(jnp.int32), -1)
    slot_ids = jnp.arange(slot_cap, dtype=jnp.int32)
    matches = position.T[:, None, :] == slot_ids[None, :, None]
    return matches.reshape(experts * slot_cap, rows).astype(jnp.bfloat16)


def shifted(value, axis, amount):
    size = lax.axis_size(axis)
    return lax.ppermute(value, axis, [(i, (i + amount) % size) for i in range(size)])


def ring_blocks(value):
    size = lax.axis_size("rep")
    up, down, blocks = value, value, [value]
    for _ in range((size - 1) // 2):
        up, down = shifted(up, "rep", 1), shifted(down, "rep", -1)
        blocks += [up, down]
    if size % 2 == 0:
        half = -(-value.shape[0] // 32) * 16
        blocks.append(shifted(up[:half], "rep", 1))
        blocks.append(shifted(down[half:], "rep", -1))
    return blocks


def back_offsets(size):
    offsets = [0]
    for distance in range(1, (size - 1) // 2 + 1):
        offsets += [distance, -distance]
    if size % 2 == 0:
        offsets.append(size // 2)
    return offsets


def grad_kernel(count, tokens_ref, *refs):
    out_ref = refs[-1]
    total, row = None, 0
    for block_ref in refs[:count]:
        rows = block_ref.shape[0]
        term = lax.dot_general(
            tokens_ref[row:row + rows, :], block_ref[...], (((0,), (0,)), ((), ())),
            preferred_element_type=jnp.float32,
        )
        total = term if total is None else total + term
        row += rows
    out_ref[...] = total.astype(out_ref.dtype)


def grad_chunk(gathered, blocks, previous, lower, hidden):
    rows, features = gathered.shape
    width = blocks[0].shape[1]
    count = len(blocks)
    in_specs = [pl.BlockSpec((rows, ROW_TILE), lambda i: (0, i))]
    in_specs += [pl.BlockSpec(b.shape, lambda i: (0, 0)) for b in blocks]
    operands, aliases = [gathered, *blocks], {}
    if previous is not None:
        in_specs.append(pl.BlockSpec(memory_space=pl.ANY))
        operands.append(previous)
        aliases = {count + 1: 0}
    place = lower // width
    return pl.pallas_call(
        functools.partial(grad_kernel, count),
        grid=(features // ROW_TILE,),
        in_specs=in_specs,
        out_specs=pl.BlockSpec((ROW_TILE, width), lambda i: (i, place)),
        out_shape=jax.ShapeDtypeStruct((features, hidden), jnp.bfloat16),
        input_output_aliases=aliases,
        compiler_params=pltpu.CompilerParams(vmem_limit_bytes=48 * 1024 * 1024),
        cost_estimate=pl.CostEstimate(
            flops=2 * rows * features * width,
            bytes_accessed=2 * (rows * (features + width) + features * width),
            transcendentals=0,
        ),
    )(*operands)


def body(tokens, routes, gate_weight, gate_cotangent):
    experts = lax.axis_size("exp")
    shards = lax.axis_size("shard")
    replicas = lax.axis_size("rep")
    features = tokens.shape[1]
    cotangent = gate_cotangent[0]
    hidden = cotangent.shape[1]
    slot_cap = cotangent.shape[0] // (experts * shards)
    weight = gate_weight[0]

    offsets = back_offsets(replicas)
    flat_routes = routes.T
    all_routes = [flat_routes if k == 0 else shifted(flat_routes, "rep", k) for k in offsets]
    all_tokens = [tokens if k == 0 else shifted(tokens, "rep", k) for k in offsets]

    bounds = [hidden * part // 7 for part in BOUNDS]
    chunks = [ring_blocks(cotangent[:, a:b]) for a, b in zip(bounds[:-1], bounds[1:])]

    partial = lax.dot_general(
        cotangent, weight, (((1,), (1,)), ((), ())), preferred_element_type=jnp.float32
    ).astype(jnp.bfloat16)
    partial = partial.reshape(experts, shards, slot_cap, features)
    me = lax.axis_index("shard")
    summed = lax.dynamic_index_in_dim(partial, me, 1, keepdims=False).astype(jnp.float32)
    for k in range(1, shards):
        leaving = lax.dynamic_index_in_dim(partial, (me + k) % shards, 1, keepdims=False)
        summed = summed + shifted(leaving, "shard", k).astype(jnp.float32)
    slot_grad = summed.astype(jnp.bfloat16)
    returned = lax.all_to_all(slot_grad, "exp", split_axis=0, concat_axis=0, tiled=True)
    placings = [slot_matrix(r.T, experts, slot_cap) for r in all_routes]
    token_grad = jnp.dot(
        placings[0].T, returned.reshape(-1, features), preferred_element_type=jnp.float32
    ).astype(jnp.bfloat16)

    outgoing = jnp.stack([
        jnp.dot(p, t, preferred_element_type=jnp.float32).astype(jnp.bfloat16)
        for p, t in zip(placings, all_tokens)
    ])
    outgoing = outgoing.reshape(replicas, experts, 1, slot_cap, features)
    copies = jnp.broadcast_to(outgoing, (replicas, experts, shards, slot_cap, features))
    copies = copies.reshape(replicas, experts * shards, slot_cap, features)
    arrived = lax.all_to_all(copies, ("exp", "shard"), split_axis=1, concat_axis=1, tiled=True)
    gathered = arrived.reshape(-1, features)

    weight_grad = None
    for lower, blocks in zip(bounds[:-1], chunks):
        weight_grad = grad_chunk(gathered, blocks, weight_grad, lower, hidden)
    return (token_grad, weight_grad[None])


def solution(mesh):
    placed = (
        P(("rep", "exp", "shard"), None),
        P(("rep", "exp", "shard"), None),
        P("exp", None, "shard"),
        P("exp", "rep", "shard"),
    )
    return jax.shard_map(
        body,
        mesh=mesh,
        in_specs=placed,
        out_specs=(P(("rep", "exp", "shard"), None), P("exp", None, "shard")),
        check_vma=False,
    )
```

```python
import functools

import jax
import jax.numpy as jnp
from jax import lax
from jax.experimental import pallas as pl
from jax.experimental.pallas import tpu as pltpu
from jax.sharding import PartitionSpec as P


ROW_TILE = 512
BOUNDS = (0, 2, 4, 6, 7)


def slot_matrix(route_rows, experts, slot_cap):
    expert_ids = jnp.arange(experts, dtype=jnp.int32)
    onehot = (route_rows[:, :, None] == expert_ids[None, None, :]).astype(jnp.int32)
    named = onehot.sum(axis=1)
    rows = named.shape[0]
    earlier = (jnp.arange(rows)[:, None] > jnp.arange(rows)[None, :]).astype(jnp.bfloat16)
    before = jnp.dot(earlier, named.astype(jnp.bfloat16), preferred_element_type=jnp.float32)
    position = jnp.where(named > 0, before.astype(jnp.int32), -1)
    slot_ids = jnp.arange(slot_cap, dtype=jnp.int32)
    matches = position.T[:, None, :] == slot_ids[None, :, None]
    return matches.reshape(experts * slot_cap, rows).astype(jnp.bfloat16)


def shifted(value, axis, amount):
    size = lax.axis_size(axis)
    return lax.ppermute(value, axis, [(i, (i + amount) % size) for i in range(size)])


def ring_blocks(value):
    size = lax.axis_size("rep")
    up, down, blocks = value, value, [value]
    for _ in range((size - 1) // 2):
        up, down = shifted(up, "rep", 1), shifted(down, "rep", -1)
        blocks += [up, down]
    if size % 2 == 0:
        half = -(-value.shape[0] // 32) * 16
        blocks.append(shifted(up[:half], "rep", 1))
        blocks.append(shifted(down[half:], "rep", -1))
    return blocks


def back_offsets(size):
    offsets = [0]
    for distance in range(1, (size - 1) // 2 + 1):
        offsets += [distance, -distance]
    if size % 2 == 0:
        offsets.append(size // 2)
    return offsets


def grad_kernel(sources, count, *refs):
    rows_refs, block_refs, out_ref = refs[:sources], refs[sources:sources + count], refs[-1]
    total, source, row = None, 0, 0
    for block_ref in block_refs:
        rows = block_ref.shape[0]
        term = lax.dot_general(
            rows_refs[source][row:row + rows, :], block_ref[...], (((0,), (0,)), ((), ())),
            preferred_element_type=jnp.float32,
        )
        total = term if total is None else total + term
        row += rows
        if row == rows_refs[source].shape[0]:
            source, row = source + 1, 0
    out_ref[...] = total.astype(out_ref.dtype)


def grad_chunk(gathered, blocks, previous, lower, hidden):
    features = gathered[0].shape[1]
    rows = sum(g.shape[0] for g in gathered)
    width = blocks[0].shape[1]
    in_specs = [pl.BlockSpec((g.shape[0], ROW_TILE), lambda i: (0, i)) for g in gathered]
    in_specs += [pl.BlockSpec(b.shape, lambda i: (0, 0)) for b in blocks]
    operands, aliases = [*gathered, *blocks], {}
    if previous is not None:
        in_specs.append(pl.BlockSpec(memory_space=pl.ANY))
        aliases = {len(operands): 0}
        operands.append(previous)
    place = lower // width
    return pl.pallas_call(
        functools.partial(grad_kernel, len(gathered), len(blocks)),
        grid=(features // ROW_TILE,),
        in_specs=in_specs,
        out_specs=pl.BlockSpec((ROW_TILE, width), lambda i: (i, place)),
        out_shape=jax.ShapeDtypeStruct((features, hidden), jnp.bfloat16),
        input_output_aliases=aliases,
        compiler_params=pltpu.CompilerParams(vmem_limit_bytes=48 * 1024 * 1024),
        cost_estimate=pl.CostEstimate(
            flops=2 * rows * features * width,
            bytes_accessed=2 * (rows * (features + width) + features * width),
            transcendentals=0,
        ),
    )(*operands)


def body(tokens, routes, gate_weight, gate_cotangent):
    experts = lax.axis_size("exp")
    shards = lax.axis_size("shard")
    replicas = lax.axis_size("rep")
    features = tokens.shape[1]
    cotangent = gate_cotangent[0]
    hidden = cotangent.shape[1]
    slot_cap = cotangent.shape[0] // (experts * shards)
    weight = gate_weight[0]

    offsets = back_offsets(replicas)
    flat_routes = routes.T
    all_routes = [flat_routes if k == 0 else shifted(flat_routes, "rep", k) for k in offsets]
    all_tokens = [tokens if k == 0 else shifted(tokens, "rep", k) for k in offsets]

    bounds = [hidden * part // 7 for part in BOUNDS]
    chunks = [ring_blocks(cotangent[:, a:b]) for a, b in zip(bounds[:-1], bounds[1:])]

    partial = lax.dot_general(
        cotangent, weight, (((1,), (1,)), ((), ())), preferred_element_type=jnp.float32
    ).astype(jnp.bfloat16)
    partial = partial.reshape(experts, shards, slot_cap, features)
    me = lax.axis_index("shard")
    summed = lax.dynamic_index_in_dim(partial, me, 1, keepdims=False).astype(jnp.float32)
    for k in range(1, shards):
        leaving = lax.dynamic_index_in_dim(partial, (me + k) % shards, 1, keepdims=False)
        summed = summed + shifted(leaving, "shard", k).astype(jnp.float32)
    slot_grad = summed.astype(jnp.bfloat16)
    returned = lax.all_to_all(slot_grad, "exp", split_axis=0, concat_axis=0, tiled=True)
    placings = [slot_matrix(r.T, experts, slot_cap) for r in all_routes]
    token_grad = jnp.dot(
        placings[0].T, returned.reshape(-1, features), preferred_element_type=jnp.float32
    ).astype(jnp.bfloat16)

    gathered = []
    for placing, rows in zip(placings, all_tokens):
        outgoing = jnp.dot(placing, rows, preferred_element_type=jnp.float32)
        outgoing = outgoing.astype(jnp.bfloat16).reshape(experts, 1, slot_cap, features)
        copies = jnp.broadcast_to(outgoing, (experts, shards, slot_cap, features))
        copies = copies.reshape(experts * shards, slot_cap, features)
        arrived = lax.all_to_all(copies, ("exp", "shard"), split_axis=0, concat_axis=0, tiled=True)
        gathered.append(arrived.reshape(-1, features))

    weight_grad = None
    for lower, blocks in zip(bounds[:-1], chunks):
        weight_grad = grad_chunk(gathered, blocks, weight_grad, lower, hidden)
    return (token_grad, weight_grad[None])


def solution(mesh):
    placed = (
        P(("rep", "exp", "shard"), None),
        P(("rep", "exp", "shard"), None),
        P("exp", None, "shard"),
        P("exp", "rep", "shard"),
    )
    return jax.shard_map(
        body,
        mesh=mesh,
        in_specs=placed,
        out_specs=(P(("rep", "exp", "shard"), None), P("exp", None, "shard")),
        check_vma=False,
    )
```
